32 devices in a mesh: prow: 8 (over z, x), pcol: 4 (over y, core).
Axes of the slice: x: 2, y: 2, z: 4, core: 2. Of those that a mesh axis runs over, the one named last changes fastest.
Arguments:
- matrix: float32 [16384, 16384], P('prow', 'pcol'), may hold values from -6 to 6
Outputs:
- reduced: float32 [16384, 16384], P('prow', 'pcol')
- householder_coefficients: float32 [2, 8], replicated
The draws below stay inside these ranges and needn't reach their ends.
All inputs are finite; a program needn't handle non-finite values.
Results may differ from the reference program's by a relative error of at most 0.0003.
Values sent between devices are 32-bit elements; how exact they have to be, the bound alone decides.
A program may use at most 128 MiB of HBM per device.

```python
import jax
import jax.numpy as jnp
from jax import lax

N = 16384
NB = 8
WINDOWS = 1


def block_scale(stream_key, shape, shards, low, high):
    loudness, own = 1.0, jax.random.fold_in(stream_key, 6)
    for dim, shards_of in shards:
        steps = jnp.exp(jax.random.uniform(jax.random.fold_in(own, dim), (shards_of,), jnp.float32, low / len(shards), high / len(shards)))
        loudness = loudness * jnp.repeat(steps, shape[dim] // shards_of).reshape([-1 if axis == dim else 1 for axis in range(len(shape))])
    return loudness


def normal_values(key, shape, spread, most, shards=(), kind=jnp.bfloat16):
    level = block_scale(key, shape, shards, -0.22, 0.18) if shards else 1.0
    values = jax.random.normal(key, shape, jnp.float32) * spread * level
    return jnp.minimum(jnp.maximum(values, -most), most).astype(kind)


def setup_inputs(seed: int = 0) -> dict:
    streams_of = jax.random.split(jax.random.key(seed), 2)
    matrix = normal_values(streams_of[0], (N, N), 1.0, 6.0, ((0, 8), (1, 4)), jnp.float32)
    return {"matrix": matrix}


epsilon = 1e-06

def precise_dot(left, right):
    return jnp.dot(left, right, precision=lax.Precision.HIGHEST)

def householder(alpha_value, sumsq):
    norm_value = jnp.sqrt(sumsq + epsilon)
    signum = jnp.where(alpha_value >= 0.0, 1.0, -1.0).astype(jnp.float32)
    beta_value = -signum * norm_value
    return (beta_value, (beta_value - alpha_value) / beta_value, alpha_value - beta_value)

def reference(matrix):
    row_index = jnp.arange(N, dtype=jnp.int32)
    col_index = jnp.arange(N, dtype=jnp.int32)
    panel_index = jnp.arange(NB, dtype=jnp.int32)
    working_array = matrix
    source_side_factor_list = []
    target_side_factor_list = []
    for window in range(WINDOWS):
        offset = window * NB
        v_rows = jnp.zeros((NB, N), jnp.float32)
        x_rows = jnp.zeros((NB, N), jnp.float32)
        y_cols = jnp.zeros((NB, N), jnp.float32)
        u_cols = jnp.zeros((NB, N), jnp.float32)
        diagonal_entries = []
        super_list = []
        for i in range(NB):
            k = offset + i
            column = working_array[:, k] - precise_dot(y_cols[:, k], v_rows) - precise_dot(u_cols[:, k], x_rows)
            masked = jnp.where(row_index >= k, column, 0.0)
            beta_left, source_side_coefficient, denom_left = householder(column[k], jnp.sum(masked * masked))
            v_new = (masked - beta_left * (row_index == k).astype(jnp.float32)) / denom_left
            transposed = precise_dot(v_new, working_array) - precise_dot(precise_dot(v_rows, v_new), y_cols) - precise_dot(precise_dot(x_rows, v_new), u_cols)
            y_new = jnp.where(col_index > k, source_side_coefficient * transposed, 0.0)
            v_rows = v_rows.at[i].set(v_new)
            y_cols = y_cols.at[i].set(y_new)
            row_eff = working_array[k, :] - precise_dot(v_rows[:, k], y_cols) - precise_dot(x_rows[:, k], u_cols)
            row_masked = jnp.where(col_index >= k + 1, row_eff, 0.0)
            right_reflector_beta, target_side_coefficient, denom_right = householder(row_eff[k + 1], jnp.sum(row_masked * row_masked))
            u_new = (row_masked - right_reflector_beta * (col_index == k + 1).astype(jnp.float32)) / denom_right
            product = precise_dot(working_array, u_new) - precise_dot(precise_dot(y_cols, u_new), v_rows) - precise_dot(precise_dot(u_cols, u_new), x_rows)
            x_new = jnp.where(row_index > k, target_side_coefficient * product, 0.0)
            x_rows = x_rows.at[i].set(x_new)
            u_cols = u_cols.at[i].set(u_new)
            diagonal_entries.append(beta_left)
            super_list.append(right_reflector_beta)
            source_side_factor_list.append(source_side_coefficient)
            target_side_factor_list.append(target_side_coefficient)
        stack_left = jnp.concatenate([v_rows, x_rows], axis=0)
        stack_right = jnp.concatenate([y_cols, u_cols], axis=0)
        updated = working_array - lax.dot_general(stack_left, stack_right, (((0,), (0,)), ((), ())), precision=lax.Precision.HIGHEST)
        updated = updated.at[offset + NB:, offset:offset + NB].set(v_rows[:, offset + NB:].T)
        row_glob = (offset + panel_index)[:, None]
        col_g = col_index[None, :]
        v_window = jnp.where(panel_index[None, :] < panel_index[:, None], v_rows[:, offset:offset + NB].T, 0.0)
        v_part = jnp.zeros((NB, N), jnp.float32).at[:, offset:offset + NB].set(v_window)
        diag_arr = jnp.stack(diagonal_entries)[:, None]
        super_arr = jnp.stack(super_list)[:, None]
        panel_values = jnp.where(col_g < offset, updated[offset:offset + NB, :], jnp.where(col_g < row_glob, v_part, jnp.where(col_g == row_glob, diag_arr, jnp.where(col_g == row_glob + 1, super_arr, u_cols))))
        working_array = updated.at[offset:offset + NB, :].set(panel_values)
    householder_coefficients = jnp.stack([jnp.stack(source_side_factor_list), jnp.stack(target_side_factor_list)])
    return (working_array, householder_coefficients)
```

```python
import functools

import jax
import jax.numpy as jnp
from jax import lax
from jax.experimental import pallas as pl
from jax.experimental.pallas import tpu as pltpu
from jax.sharding import PartitionSpec as P

NB = 8
EPS = 1e-06
LANES = 128
Y_PARTS = (1, 2, 3, 2)
XC = 2
UPDATE_ROWS = 128
MESH = pl.DeviceIdType.MESH


def householder(alpha, sumsq):
    beta = jnp.where(alpha >= 0.0, -1.0, 1.0) * jnp.sqrt(sumsq + EPS)
    return beta, (beta - alpha) / beta, alpha - beta


def lane_sum(x):
    return jnp.sum(x, axis=1, keepdims=True)


def total(x):
    return jnp.sum(lane_sum(x), axis=0, keepdims=True)


def y_chunks(cs):
    unit = cs // sum(Y_PARTS)
    sizes = [unit * part for part in Y_PARTS]
    return [(sum(sizes[:c]), n) for c, n in enumerate(sizes)]


def peers(me, n):
    if n & (n - 1):
        return [(d, lax.rem(me + d, n)) for d in range(1, n)]
    out = []
    for m in range(n - 1, 0, -1):
        other = me
        for b in range(n.bit_length() - 1):
            if m >> b & 1:
                other = other + (1 - 2 * lax.rem(me // (1 << b), 2)) * (1 << b)
        out.append((m, other))
    return out


def panel_kernel(np_, nq, a_hbm, a, left_o, right_o, scal_o,
                 strip, arows, colp, rowp, v_s, x_s, y_s, u_s, vb, ub, acc_s,
                 ybuf, xbuf, column_s,
                 a_sem, strip_sem, arow_sem, col_ssem, col_rsem, row_ssem, row_rsem,
                 y_ssem, y_rsem, x_ssem, x_rsem):
    me_p = lax.axis_index("prow")
    me_q = lax.axis_index("pcol")
    rows, cols = a.shape
    rs, cs = rows // LANES, cols // LANES
    ych = y_chunks(cs)
    xper = rs // XC
    groups = LANES // 8
    p_peers, q_peers = peers(me_p, np_), peers(me_q, nq)

    strip_cp = pltpu.make_async_copy(a_hbm.at[:, pl.ds(0, LANES)], strip, strip_sem)
    strip_cp.start()
    arow_cp = pltpu.make_async_copy(a_hbm.at[pl.ds(0, NB), :], arows, arow_sem)
    arow_cp.start()
    a_cps = []
    for c, (lo, n) in enumerate(ych):
        part = pl.ds(lo * LANES, n * LANES)
        cp = pltpu.make_async_copy(a_hbm.at[:, part], a.at[:, part], a_sem.at[c])
        cp.start()
        a_cps.append(cp)

    barrier = pltpu.get_barrier_semaphore()
    for d in range(1, np_):
        pl.semaphore_signal(barrier, inc=1, device_id={"prow": lax.rem(me_p + d, np_)}, device_id_type=MESH)
    for d in range(1, nq):
        pl.semaphore_signal(barrier, inc=1, device_id={"pcol": lax.rem(me_q + d, nq)}, device_id_type=MESH)
    pl.semaphore_wait(barrier, np_ + nq - 2)

    lane8 = lax.broadcasted_iota(jnp.int32, (8, LANES), 1)
    sub8 = lax.broadcasted_iota(jnp.int32, (8, LANES), 0)
    row_gl = (me_p * rows + lax.broadcasted_iota(jnp.int32, (rs, LANES), 0) * LANES
              + lax.broadcasted_iota(jnp.int32, (rs, LANES), 1))

    def col_gl(lo, n):
        return (me_q * cols + (lo + lax.broadcasted_iota(jnp.int32, (n, LANES), 0)) * LANES
                + lax.broadcasted_iota(jnp.int32, (n, LANES), 1))

    strip_cp.wait()
    arow_cp.wait()

    def col_copy(d):
        return pltpu.make_async_remote_copy(
            src_ref=colp, dst_ref=colp, send_sem=col_ssem.at[d], recv_sem=col_rsem,
            device_id={"pcol": lax.rem(me_q + d, nq)}, device_id_type=MESH)

    def row_copy(i, d):
        return pltpu.make_async_remote_copy(
            src_ref=rowp.at[i], dst_ref=rowp.at[i], send_sem=row_ssem.at[i, d], recv_sem=row_rsem.at[i],
            device_id={"prow": lax.rem(me_p + d, np_)}, device_id_type=MESH)

    @pl.when(me_q == 0)
    def _():
        @pl.loop(0, rs)
        def _(s):
            t = strip[pl.ds(s * LANES, LANES), :].T
            for c in range(NB + 1):
                colp[c, pl.ds(s, 1), :] = t[c:c + 1, :]
        for d in range(1, nq):
            col_copy(d).start()

    @pl.when(me_p == 0)
    def _():
        for s in range(cs):
            blk = arows[:, s * LANES:(s + 1) * LANES]
            for i in range(NB):
                rowp[i, s:s + 1, :] = blk[i:i + 1, :]
        for i in range(2):
            for d in range(1, np_):
                row_copy(i, d).start()

    for ref in (v_s, x_s, y_s, u_s):
        ref[...] = jnp.zeros(ref.shape, jnp.float32)

    @pl.when(me_q != 0)
    def _():
        col_copy(1).wait_recv()

    column_s[...] = colp[0]

    def y_copy(i, m, peer, c):
        lo, n = ych[c]
        lo, n = (0, 8 + n) if c == 0 else (8 + lo, n)
        ref = ybuf.at[i, me_p, pl.ds(lo, n), :]
        return pltpu.make_async_remote_copy(
            src_ref=ref, dst_ref=ref, send_sem=y_ssem.at[m, c], recv_sem=y_rsem.at[lax.rem(i, 2), m, c],
            device_id={"prow": peer}, device_id_type=MESH)

    def x_copy(i, m, peer, c):
        lo, n = (0, 8 + xper) if c == 0 else (8 + c * xper, xper)
        ref = xbuf.at[i, me_q, pl.ds(lo, n), :]
        return pltpu.make_async_remote_copy(
            src_ref=ref, dst_ref=ref, send_sem=x_ssem.at[m, c], recv_sem=x_rsem.at[lax.rem(i, 2), m, c],
            device_id={"pcol": peer}, device_id_type=MESH)

    def scalar_tile(first, second, vec, here, at):
        tile = jnp.zeros((8, LANES), jnp.float32)
        for k, ref in enumerate((first, second)):
            tile = jnp.where(lane8 == k, lane_sum(jnp.sum(ref[...] * vec[None], axis=1)), tile)
        hit = jnp.logical_and(here, lane8 == at)
        for k, ref in enumerate((first, second)):
            tile = jnp.where(lane8 == 2 + k, lane_sum(jnp.where(hit, ref[:, 0, :], 0.0)), tile)
        alpha = lane_sum(jnp.where(hit[0:1], vec[0:1], 0.0))
        s = jnp.where(sub8[:, :1] == 0, alpha, total(vec * vec))
        return jnp.where(lane8 == 4, s, tile)

    def unpack(tile):
        return [jnp.broadcast_to(lane_sum(jnp.where(lane8 == k, tile, 0.0)), (8, LANES)) for k in range(5)]

    def combine(coef_a, ref_a, coef_b, ref_b, lo, n):
        part = pl.ds(lo, n)
        acc = coef_a[0:1] * ref_a[0, part, :] + coef_b[0:1] * ref_b[0, part, :]
        for j in range(1, NB):
            acc = acc + (coef_a[j:j + 1] * ref_a[j, part, :] + coef_b[j:j + 1] * ref_b[j, part, :])
        return acc

    def spread(s):
        row = jnp.broadcast_to(column_s[s:s + 1, :], (8, LANES))
        return [jnp.broadcast_to(lane_sum(jnp.where(lane8 == sub8 + 8 * g, row, 0.0)), (8, LANES))
                for g in range(groups)]

    def y_finish(i, c, accs):
        lo, n = ych[c]
        for j in range(n):
            t = 8 + lo + j
            ybuf[i, me_p, t:t + 1, :] = jnp.sum(accs[j] + accs[n + j], axis=0, keepdims=True)
        for m, peer in p_peers:
            y_copy(i, m, peer, c).start()

    @pl.loop(0, NB)
    def _(i):
        masked = jnp.where(row_gl >= i, column_s[...], 0.0)
        unit_r = (row_gl == i).astype(jnp.float32)
        column_s[...] = masked
        ybuf[i, me_p, 0:8, :] = scalar_tile(v_s, x_s, masked, me_p == 0, i)

        for c, (lo, n) in enumerate(ych):
            @pl.when(i == 0)
            def _(c=c):
                a_cps[c].wait()

            if c == 0:
                accs = [jnp.zeros((8, LANES), jnp.float32)] * (2 * n)
                for s in range(rs):
                    for g, v in enumerate(spread(s)):
                        r = pl.ds(s * LANES + 8 * g, 8)
                        vb[r, :] = v
                        for j in range(n):
                            m = (g % 2) * n + j
                            accs[m] = accs[m] + v * a[r, (lo + j) * LANES:(lo + j + 1) * LANES]
            else:
                def body(s, accs, lo=lo, n=n):
                    accs = list(accs)
                    for g in range(groups):
                        r = pl.ds(pl.multiple_of(s * LANES + 8 * g, 8), 8)
                        v = vb[r, :]
                        for j in range(n):
                            m = (g % 2) * n + j
                            accs[m] = accs[m] + v * a[r, (lo + j) * LANES:(lo + j + 1) * LANES]
                    return tuple(accs)

                accs = lax.fori_loop(0, rs, body, (jnp.zeros((8, LANES), jnp.float32),) * (2 * n))
            y_finish(i, c, accs)

        @pl.when(jnp.logical_and(me_p == 0, i < NB - 2))
        def _():
            for d in range(1, np_):
                row_copy(i + 2, d).start()

        @pl.when(me_p != 0)
        def _():
            row_copy(i, 1).wait_recv()

        for c, (lo, n) in enumerate(ych):
            for m, peer in p_peers:
                y_copy(i, m, peer, c).wait_recv()
            if c == 0:
                tile = ybuf[i, 0, 0:8, :]
                for p in range(1, np_):
                    tile = tile + ybuf[i, p, 0:8, :]
                v_coef, x_coef, v_at, x_at, misc = unpack(tile)
                beta, tau, denom = householder(misc[0:1], misc[1:2])
                inv = 1.0 / denom
                v_s[i] = (masked - beta * unit_r) * inv
                scal_o[0, pl.ds(i, 1), :] = beta
                scal_o[2, pl.ds(i, 1), :] = tau
            part, buf = pl.ds(lo, n), pl.ds(8 + lo, n)
            summed = ybuf[i, 0, buf, :]
            for p in range(1, np_):
                summed = summed + ybuf[i, p, buf, :]
            row_eff = rowp[i, part, :] - combine(v_at, y_s, x_at, u_s, lo, n)
            trans = (summed - combine(v_coef, y_s, x_coef, u_s, lo, n) - beta * row_eff) * inv
            mine = col_gl(lo, n) > i
            y_new = jnp.where(mine, tau * trans, 0.0)
            y_s[i, part, :] = y_new
            ub[part, :] = jnp.where(mine, row_eff - y_new, 0.0)
            us = [jnp.broadcast_to(ub[lo + j:lo + j + 1, :], (8, LANES)) for j in range(n)]

            def product(r, us=us, lo=lo, n=n):
                p = [us[k] * a[r, (lo + k) * LANES:(lo + k + 1) * LANES] for k in range(2)]
                for j in range(2, n):
                    p[j % 2] = p[j % 2] + us[j] * a[r, (lo + j) * LANES:(lo + j + 1) * LANES]
                return p[0] + p[1]

            if c < len(ych) - 1:
                @pl.loop(0, rs)
                def _(s, c=c, product=product):
                    for g in range(groups):
                        r = pl.ds(pl.multiple_of(s * LANES + 8 * g, 8), 8)
                        acc_s[r, :] = product(r) if c == 0 else acc_s[r, :] + product(r)
            else:
                row_m = ub[...]
                xbuf[i, me_q, 0:8, :] = scalar_tile(y_s, u_s, row_m, me_q == 0, i + 1)
                for h in range(XC):
                    @pl.loop(h * xper, (h + 1) * xper, unroll=min(4, xper))
                    def _(s, product=product):
                        tile = jnp.zeros((8, LANES), jnp.float32)
                        for g in range(groups):
                            r = pl.ds(pl.multiple_of(s * LANES + 8 * g, 8), 8)
                            tile = jnp.where(lane8 == sub8 + 8 * g, lane_sum(acc_s[r, :] + product(r)), tile)
                        xbuf[i, me_q, pl.ds(8 + s, 1), :] = jnp.sum(tile, axis=0, keepdims=True)
                    for m, peer in q_peers:
                        x_copy(i, m, peer, h).start()

        for c in range(len(ych)):
            for m, peer in p_peers:
                y_copy(i, m, peer, c).wait_send()
        unit_c = (col_gl(0, cs) == i + 1).astype(jnp.float32)
        for h in range(XC):
            for m, peer in q_peers:
                x_copy(i, m, peer, h).wait()
        xsum = xbuf[i, 0]
        for q in range(1, nq):
            xsum = xsum + xbuf[i, q]
        y_coef, u_coef, y_at, u_at, misc2 = unpack(xsum[0:8])
        beta2, tau2, denom2 = householder(misc2[0:1], misc2[1:2])
        col_next = colp[i + 1] - combine(y_at, v_s, u_at, x_s, 0, rs)
        inv2 = 1.0 / denom2
        prod = (xsum[8:] - combine(y_coef, v_s, u_coef, x_s, 0, rs) - beta2 * col_next) * inv2
        x_new = jnp.where(row_gl > i, tau2 * prod, 0.0)
        x_s[i] = x_new
        u_s[i] = (row_m - beta2 * unit_c) * inv2
        scal_o[1, pl.ds(i, 1), :] = beta2
        scal_o[3, pl.ds(i, 1), :] = tau2
        column_s[...] = col_next - x_new

    for s in range(rs):
        left_o[0:NB, s * LANES:(s + 1) * LANES] = v_s[:, s, :]
        left_o[NB:, s * LANES:(s + 1) * LANES] = x_s[:, s, :]
    for s in range(cs):
        right_o[0:NB, s * LANES:(s + 1) * LANES] = y_s[:, s, :]
        right_o[NB:, s * LANES:(s + 1) * LANES] = u_s[:, s, :]

    @pl.when(me_q == 0)
    def _():
        for d in range(1, nq):
            col_copy(d).wait_send()

    @pl.when(me_p == 0)
    def _():
        @pl.loop(0, NB)
        def _(i):
            for d in range(1, np_):
                row_copy(i, d).wait_send()


def reduce_panel(matrix, np_, nq):
    rows, cols = matrix.shape
    rs, cs = rows // LANES, cols // LANES
    f32 = jnp.float32
    vmem = pl.BlockSpec(memory_space=pltpu.VMEM)
    dma = pltpu.SemaphoreType.DMA
    yc = len(Y_PARTS)
    return pl.pallas_call(
        functools.partial(panel_kernel, np_, nq),
        out_shape=(pltpu.VMEM((rows, cols), f32),
                   pltpu.VMEM((2 * NB, rows), f32),
                   pltpu.VMEM((2 * NB, cols), f32),
                   pltpu.VMEM((4, NB, LANES), f32)),
        in_specs=[pl.BlockSpec(memory_space=pl.ANY)],
        out_specs=(vmem, vmem, vmem, vmem),
        scratch_shapes=[
            pltpu.VMEM((rows, LANES), f32),
            pltpu.VMEM((NB, cols), f32),
            pltpu.VMEM((NB + 1, rs, LANES), f32),
            pltpu.VMEM((NB, cs, LANES), f32),
            pltpu.VMEM((NB, rs, LANES), f32),
            pltpu.VMEM((NB, rs, LANES), f32),
            pltpu.VMEM((NB, cs, LANES), f32),
            pltpu.VMEM((NB, cs, LANES), f32),
            pltpu.VMEM((rows, LANES), f32),
            pltpu.VMEM((cs, LANES), f32),
            pltpu.VMEM((rows, LANES), f32),
            pltpu.VMEM((NB, np_, 8 + cs, LANES), f32),
            pltpu.VMEM((NB, nq, 8 + rs, LANES), f32),
            pltpu.VMEM((rs, LANES), f32),
            dma((yc,)), dma, dma,
            dma((nq,)), dma, dma((NB, np_)), dma((NB,)),
            dma((np_, yc)), dma((2, np_, yc)), dma((nq, XC)), dma((2, nq, XC)),
        ],
        compiler_params=pltpu.CompilerParams(
            collective_id=0, has_side_effects=True, vmem_limit_bytes=20 * 1024 * 1024),
    )(matrix)


def pieces(x):
    hi = x.astype(jnp.bfloat16)
    rest = x - hi.astype(jnp.float32)
    mid = rest.astype(jnp.bfloat16)
    lo = (rest - mid.astype(jnp.float32)).astype(jnp.bfloat16)
    return hi, mid, lo


def update_kernel(a_ref, left_ref, right_ref, scal_ref, out_ref, coef_ref, left_p, right_p):
    me_p = lax.axis_index("prow")
    me_q = lax.axis_index("pcol")
    step = pl.program_id(0)
    block, cols = out_ref.shape
    dims = (((0,), (0,)), ((), ()))

    @pl.when(step == 0)
    def _():
        lh, lm, ll = pieces(left_ref[...])
        rh, rm, rl = pieces(right_ref[...])
        for k, (lp, rp) in enumerate(((lh, rh), (lh, rm), (lh, rl), (lm, rh), (lm, rm), (ll, rh))):
            left_p[2 * NB * k:2 * NB * (k + 1), :] = lp
            right_p[2 * NB * k:2 * NB * (k + 1), :] = rp
        lane = lax.broadcasted_iota(jnp.int32, (NB, LANES), 1)
        sub = lax.broadcasted_iota(jnp.int32, (NB, LANES), 0)
        for t in range(2):
            row = jnp.sum(jnp.where(lane == sub, scal_ref[2 + t], 0.0), axis=0, keepdims=True)
            coef_ref[t:t + 1, :] = row[:, 0:NB]

    left = left_p[:, pl.ds(pl.multiple_of(step * block, block), block)]
    rows = pl.ds(pl.multiple_of(step * block, block), block)
    out_ref[...] = a_ref[rows, :] - lax.dot_general(
        left, right_p[...], dims, preferred_element_type=jnp.float32)

    @pl.when(me_q == 0)
    def _():
        k = left.shape[0]
        src = lax.broadcasted_iota(jnp.int32, (k, LANES), 0)
        lane = lax.broadcasted_iota(jnp.int32, (k, LANES), 1)
        pick = jnp.logical_and(
            lane < NB, (src == lane) | (src == lane + 6 * NB) | (src == lane + 10 * NB))
        vt = lax.dot_general(left, jnp.where(pick, 1.0, 0.0).astype(jnp.bfloat16), dims,
                             preferred_element_type=jnp.float32)
        lanes = lax.broadcasted_iota(jnp.int32, (block, LANES), 1)
        out_ref[:, 0:LANES] = jnp.where(lanes < NB, vt, out_ref[:, 0:LANES])

    @pl.when(jnp.logical_and(me_p == 0, step == 0))
    def _():
        vt = out_ref[0:NB, 0:LANES]
        out_ref[0:NB, :] = right_ref[NB:, :]

        @pl.when(me_q == 0)
        def _():
            r = lax.broadcasted_iota(jnp.int32, (NB, LANES), 0)
            c = lax.broadcasted_iota(jnp.int32, (NB, LANES), 1)
            out_ref[0:NB, 0:LANES] = jnp.where(
                c < r, vt,
                jnp.where(c == r, scal_ref[0], jnp.where(c == r + 1, scal_ref[1], right_ref[NB:, 0:LANES])))


def apply_panel(matrix, left, right, scal):
    rows, cols = matrix.shape
    block = min(rows, UPDATE_ROWS)
    vmem = pl.BlockSpec(memory_space=pltpu.VMEM)
    return pl.pallas_call(
        update_kernel,
        out_shape=(jax.ShapeDtypeStruct((rows, cols), jnp.float32),
                   jax.ShapeDtypeStruct((2, NB), jnp.float32)),
        grid=(rows // block,),
        in_specs=[vmem, vmem, vmem, vmem],
        out_specs=(pl.BlockSpec((block, cols), lambda i: (i, 0)),
                   pl.BlockSpec((2, NB), lambda i: (0, 0))),
        scratch_shapes=[pltpu.VMEM((12 * NB, rows), jnp.bfloat16),
                        pltpu.VMEM((12 * NB, cols), jnp.bfloat16)],
        compiler_params=pltpu.CompilerParams(vmem_limit_bytes=20 * 1024 * 1024),
    )(matrix, left, right, scal)


def solution(mesh):
    np_, nq = mesh.shape["prow"], mesh.shape["pcol"]

    def per_device(matrix):
        return apply_panel(*reduce_panel(matrix, np_, nq))

    return jax.shard_map(
        per_device, mesh=mesh, in_specs=(P("prow", "pcol"),),
        out_specs=(P("prow", "pcol"), P()), check_vma=False)
```

```python
import functools

import jax
import jax.numpy as jnp
from jax import lax
from jax.experimental import pallas as pl
from jax.experimental.pallas import tpu as pltpu
from jax.sharding import PartitionSpec as P

NB = 8
EPS = 1e-06
LANES = 128
Y_PARTS = (1, 2, 2, 2, 1)
UPDATE_ROWS = 128
UPDATE_SLOTS = 6
BLOCKS = 2
MESH = pl.DeviceIdType.MESH


def householder(alpha, sumsq):
    beta = jnp.where(alpha >= 0.0, -1.0, 1.0) * jnp.sqrt(sumsq + EPS)
    return beta, (beta - alpha) / beta, alpha - beta


def lane_sum(x):
    return jnp.sum(x, axis=1, keepdims=True)


def total(x):
    return jnp.sum(lane_sum(x), axis=0, keepdims=True)


def y_chunks(cs):
    unit = cs // sum(Y_PARTS)
    sizes = [unit * part for part in Y_PARTS]
    return [(sum(sizes[:c]), n) for c, n in enumerate(sizes)]


def peers(me, n):
    if n & (n - 1):
        return [(d, lax.rem(me + d, n)) for d in range(1, n)]
    out = []
    for m in range(n - 1, 0, -1):
        other = me
        for b in range(n.bit_length() - 1):
            if m >> b & 1:
                other = other + (1 - 2 * lax.rem(me // (1 << b), 2)) * (1 << b)
        out.append((m, other))
    return out


def panel_kernel(np_, nq, a_hbm, a, left_o, right_o, scal_o,
                 strip, arows, colp, rowp, v_s, x_s, y_s, u_s, vb, ub, acc_s,
                 ybuf, xbuf, column_s,
                 a_sem, strip_sem, arow_sem, col_ssem, col_rsem, row_ssem, row_rsem,
                 y_ssem, y_rsem, x_ssem, x_rsem):
    me_p = lax.axis_index("prow")
    me_q = lax.axis_index("pcol")
    rows, cols = a.shape
    rs, cs = rows // LANES, cols // LANES
    ych = y_chunks(cs)
    groups = LANES // 8
    p_peers, q_peers = peers(me_p, np_), peers(me_q, nq)

    strip_cp = pltpu.make_async_copy(a_hbm.at[:, pl.ds(0, LANES)], strip, strip_sem)
    strip_cp.start()
    arow_cp = pltpu.make_async_copy(a_hbm.at[pl.ds(0, NB), :], arows, arow_sem)
    arow_cp.start()
    a_cps = []
    for c, (lo, n) in enumerate(ych):
        part = pl.ds(lo * LANES, n * LANES)
        a_cps.append(pltpu.make_async_copy(a_hbm.at[:, part], a.at[:, part], a_sem.at[c]))
    for cp in a_cps[:2]:
        cp.start()

    barrier = pltpu.get_barrier_semaphore()
    for d in range(1, np_):
        pl.semaphore_signal(barrier, inc=1, device_id={"prow": lax.rem(me_p + d, np_)}, device_id_type=MESH)
    for d in range(1, nq):
        pl.semaphore_signal(barrier, inc=1, device_id={"pcol": lax.rem(me_q + d, nq)}, device_id_type=MESH)
    pl.semaphore_wait(barrier, np_ + nq - 2)

    lane8 = lax.broadcasted_iota(jnp.int32, (8, LANES), 1)
    sub8 = lax.broadcasted_iota(jnp.int32, (8, LANES), 0)
    row_gl = (me_p * rows + lax.broadcasted_iota(jnp.int32, (rs, LANES), 0) * LANES
              + lax.broadcasted_iota(jnp.int32, (rs, LANES), 1))

    def col_gl(lo, n):
        return (me_q * cols + (lo + lax.broadcasted_iota(jnp.int32, (n, LANES), 0)) * LANES
                + lax.broadcasted_iota(jnp.int32, (n, LANES), 1))

    def col_copy(h, d):
        part = colp.at[pl.ds(0, 1)] if h == 0 else colp.at[pl.ds(1, NB)]
        return pltpu.make_async_remote_copy(
            src_ref=part, dst_ref=part, send_sem=col_ssem.at[h, d], recv_sem=col_rsem.at[h],
            device_id={"pcol": lax.rem(me_q + d, nq)}, device_id_type=MESH)

    def row_copy(i, d):
        return pltpu.make_async_remote_copy(
            src_ref=rowp.at[i], dst_ref=rowp.at[i], send_sem=row_ssem.at[i, d], recv_sem=row_rsem.at[i],
            device_id={"prow": lax.rem(me_p + d, np_)}, device_id_type=MESH)

    strip_cp.wait()

    @pl.when(me_q == 0)
    def _():
        @pl.loop(0, rs, unroll=min(8, rs))
        def _(s):
            t = strip[pl.ds(s * LANES, LANES), :].T
            for c in range(NB + 1):
                colp[c, pl.ds(s, 1), :] = t[c:c + 1, :]
        for h in range(2):
            for d in range(1, nq):
                col_copy(h, d).start()

    arow_cp.wait()

    @pl.when(me_p == 0)
    def _():
        for s in range(cs):
            blk = arows[:, s * LANES:(s + 1) * LANES]
            for i in range(NB):
                rowp[i, s:s + 1, :] = blk[i:i + 1, :]
        for i in range(2):
            for d in range(1, np_):
                row_copy(i, d).start()

    for cp in a_cps[2:]:
        cp.start()

    for ref in (v_s, x_s, y_s, u_s, left_o, right_o):
        ref[...] = jnp.zeros(ref.shape, jnp.float32)

    @pl.when(me_q != 0)
    def _():
        col_copy(0, 1).wait_recv()

    column_s[...] = colp[0]

    def y_part(c):
        lo, n = ych[c]
        return pl.ds(7, 1 + n) if c == 0 else pl.ds(8 + lo, n)

    def y_send(i, c):
        ref = ybuf.at[i, me_p, y_part(c), :]
        for m, peer in p_peers:
            pltpu.make_async_remote_copy(
                src_ref=ref, dst_ref=ref, send_sem=y_ssem.at[c], recv_sem=y_rsem.at[lax.rem(i, 2), c],
                device_id={"prow": peer}, device_id_type=MESH).start()

    def y_wait(i, c, sem):
        ref = ybuf.at[i, pl.ds(0, np_ - 1), y_part(c), :]
        pltpu.make_async_copy(ref, ref, sem).wait()

    def x_send(i):
        ref = xbuf.at[i, me_q, pl.ds(7, 1 + rs), :]
        for m, peer in q_peers:
            pltpu.make_async_remote_copy(
                src_ref=ref, dst_ref=ref, send_sem=x_ssem, recv_sem=x_rsem.at[lax.rem(i, 2)],
                device_id={"pcol": peer}, device_id_type=MESH).start()

    def x_wait(i, sem):
        ref = xbuf.at[i, pl.ds(0, nq - 1), pl.ds(7, 1 + rs), :]
        pltpu.make_async_copy(ref, ref, sem).wait()

    def scalar_row(first, second, vec, here, at):
        sums = [lane_sum(jnp.sum(ref[...] * vec[None], axis=1)) for ref in (first, second)]
        hit = jnp.logical_and(here, lane8 == at)
        sums += [lane_sum(jnp.where(hit, ref[:, 0, :], 0.0)) for ref in (first, second)]
        alpha = lane_sum(jnp.where(hit[0:1], vec[0:1], 0.0))
        sums.append(jnp.where(sub8[:, :1] == 0, alpha, total(vec * vec)))
        tile = jnp.zeros((8, LANES), jnp.float32)
        for k, one in enumerate(sums):
            tile = jnp.where(lane8 == sub8 + 8 * k, one, tile)
        return jnp.sum(tile, axis=0, keepdims=True)

    def unpack(buf, n):
        row = buf[0, 7:8, :]
        for p in range(1, n):
            row = row + buf[p, 7:8, :]
        row = jnp.broadcast_to(row, (8, LANES))
        return [jnp.broadcast_to(lane_sum(jnp.where(lane8 == sub8 + 8 * k, row, 0.0)), (8, LANES))
                for k in range(5)]

    def combine(coef_a, ref_a, coef_b, ref_b, lo, n):
        part = pl.ds(lo, n)
        acc = coef_a[0:1] * ref_a[0, part, :] + coef_b[0:1] * ref_b[0, part, :]
        for j in range(1, NB):
            acc = acc + (coef_a[j:j + 1] * ref_a[j, part, :] + coef_b[j:j + 1] * ref_b[j, part, :])
        return acc

    def spread(s):
        row = jnp.broadcast_to(column_s[s:s + 1, :], (8, LANES))
        return [jnp.broadcast_to(lane_sum(jnp.where(lane8 == sub8 + 8 * g, row, 0.0)), (8, LANES))
                for g in range(groups)]

    def y_finish(i, c, accs):
        lo, n = ych[c]
        for j in range(n):
            t = 8 + lo + j
            ybuf[i, me_p, t:t + 1, :] = jnp.sum(accs[j] + accs[n + j], axis=0, keepdims=True)
        y_send(i, c)

    def y_block(s, c, accs):
        lo, n = ych[c]
        accs = list(accs)
        for g in range(BLOCKS * groups):
            r = pl.ds(pl.multiple_of(s * (BLOCKS * LANES) + 8 * g, 8), 8)
            v = vb[r, :]
            for j in range(n):
                m = (g % 2) * n + j
                accs[m] = accs[m] + v * a[r, (lo + j) * LANES:(lo + j + 1) * LANES]
        return tuple(accs)

    def put(out, base, i, ref):
        for s in range(ref.shape[1]):
            part = slice(s * LANES, (s + 1) * LANES)
            row = jnp.broadcast_to(ref[i, s:s + 1, :], (NB, LANES))
            out[base:base + NB, part] = jnp.where(sub8 == i, row, out[base:base + NB, part])

    @pl.loop(0, NB)
    def _(i):
        masked = jnp.where(row_gl >= i, column_s[...], 0.0)
        unit_r = (row_gl == i).astype(jnp.float32)
        column_s[...] = masked

        @pl.when(i == 0)
        def _():
            a_cps[0].wait()

        ybuf[i, me_p, 7:8, :] = scalar_row(v_s, x_s, masked, me_p == 0, i)
        lo, n = ych[0]
        accs = [jnp.zeros((8, LANES), jnp.float32)] * (2 * n)
        for s in range(rs):
            for g, v in enumerate(spread(s)):
                r = pl.ds(s * LANES + 8 * g, 8)
                vb[r, :] = v
                for j in range(n):
                    m = (g % 2) * n + j
                    accs[m] = accs[m] + v * a[r, (lo + j) * LANES:(lo + j + 1) * LANES]
        for c in range(1, len(ych)):
            @pl.when(i == 0)
            def _(c=c):
                a_cps[c].wait()

            y_finish(i, c - 1, accs)
            zeros = (jnp.zeros((8, LANES), jnp.float32),) * (2 * ych[c][1])
            accs = lax.fori_loop(1, rs // BLOCKS, functools.partial(lambda s, t, c: y_block(s, c, t), c=c),
                                 y_block(0, c, zeros))
        y_finish(i, len(ych) - 1, accs)

        @pl.when(me_p != 0)
        def _():
            row_copy(i, 1).wait_recv()

        for c, (lo, n) in enumerate(ych):
            y_wait(i, c, y_rsem.at[lax.rem(i, 2), c])
            if c == 0:
                v_coef, x_coef, v_at, x_at, misc = unpack(ybuf.at[i], np_)
                beta, tau, denom = householder(misc[0:1], misc[1:2])
                inv = 1.0 / denom
                v_s[i] = (masked - beta * unit_r) * inv
                scal_o[0, pl.ds(i, 1), :] = beta
                scal_o[2, pl.ds(i, 1), :] = tau
            part, buf = pl.ds(lo, n), pl.ds(8 + lo, n)
            summed = ybuf[i, 0, buf, :]
            for p in range(1, np_):
                summed = summed + ybuf[i, p, buf, :]
            row_eff = rowp[i, part, :] - combine(v_at, y_s, x_at, u_s, lo, n)
            trans = (summed - combine(v_coef, y_s, x_coef, u_s, lo, n) - beta * row_eff) * inv
            mine = col_gl(lo, n) > i
            y_new = jnp.where(mine, tau * trans, 0.0)
            y_s[i, part, :] = y_new
            ub[part, :] = jnp.where(mine, row_eff - y_new, 0.0)
            us = [jnp.broadcast_to(ub[lo + j:lo + j + 1, :], (8, LANES)) for j in range(n)]

            def product(r, us=us, lo=lo, n=n):
                p = [us[k] * a[r, (lo + k) * LANES:(lo + k + 1) * LANES] for k in range(2)]
                for j in range(2, n):
                    p[j % 2] = p[j % 2] + us[j] * a[r, (lo + j) * LANES:(lo + j + 1) * LANES]
                return p[0] + p[1]

            if c < len(ych) - 1:
                @pl.loop(0, rs // BLOCKS)
                def _(s, c=c, product=product):
                    for g in range(BLOCKS * groups):
                        r = pl.ds(pl.multiple_of(s * (BLOCKS * LANES) + 8 * g, 8), 8)
                        acc_s[r, :] = product(r) if c == 0 else acc_s[r, :] + product(r)
            else:
                row_m = ub[...]
                xbuf[i, me_q, 7:8, :] = scalar_row(y_s, u_s, row_m, me_q == 0, i + 1)
                for s in range(rs):
                    tile = jnp.zeros((8, LANES), jnp.float32)
                    for g in range(groups):
                        r = pl.ds(s * LANES + 8 * g, 8)
                        tile = jnp.where(lane8 == sub8 + 8 * g, lane_sum(acc_s[r, :] + product(r)), tile)
                    xbuf[i, me_q, 8 + s:9 + s, :] = jnp.sum(tile, axis=0, keepdims=True)
                x_send(i)

        @pl.when(jnp.logical_and(me_p == 0, i < NB - 2))
        def _():
            for d in range(1, np_):
                row_copy(i + 2, d).start()

        @pl.when(jnp.logical_and(me_q != 0, i == 0))
        def _():
            col_copy(1, 1).wait_recv()

        for c in range(len(ych)):
            y_wait(i, c, y_ssem.at[c])
        put(left_o, 0, i, v_s)
        put(right_o, 0, i, y_s)

        @pl.when(i > 0)
        def _():
            put(left_o, NB, i - 1, x_s)
            put(right_o, NB, i - 1, u_s)

        unit_c = (col_gl(0, cs) == i + 1).astype(jnp.float32)
        x_wait(i, x_ssem)
        x_wait(i, x_rsem.at[lax.rem(i, 2)])
        y_coef, u_coef, y_at, u_at, misc2 = unpack(xbuf.at[i], nq)
        xsum = xbuf[i, 0, 8:8 + rs, :]
        for q in range(1, nq):
            xsum = xsum + xbuf[i, q, 8:8 + rs, :]
        beta2, tau2, denom2 = householder(misc2[0:1], misc2[1:2])
        col_next = colp[i + 1] - combine(y_at, v_s, u_at, x_s, 0, rs)
        inv2 = 1.0 / denom2
        prod = (xsum - combine(y_coef, v_s, u_coef, x_s, 0, rs) - beta2 * col_next) * inv2
        x_new = jnp.where(row_gl > i, tau2 * prod, 0.0)
        x_s[i] = x_new
        u_s[i] = (row_m - beta2 * unit_c) * inv2
        scal_o[1, pl.ds(i, 1), :] = beta2
        scal_o[3, pl.ds(i, 1), :] = tau2
        column_s[...] = col_next - x_new

    put(left_o, NB, NB - 1, x_s)
    put(right_o, NB, NB - 1, u_s)

    @pl.when(me_q == 0)
    def _():
        for h in range(2):
            for d in range(1, nq):
                col_copy(h, d).wait_send()

    @pl.when(me_p == 0)
    def _():
        @pl.loop(0, NB)
        def _(i):
            for d in range(1, np_):
                row_copy(i, d).wait_send()


def reduce_panel(matrix, np_, nq):
    rows, cols = matrix.shape
    rs, cs = rows // LANES, cols // LANES
    f32 = jnp.float32
    vmem = pl.BlockSpec(memory_space=pltpu.VMEM)
    dma = pltpu.SemaphoreType.DMA
    yc = len(Y_PARTS)
    return pl.pallas_call(
        functools.partial(panel_kernel, np_, nq),
        out_shape=(pltpu.VMEM((rows, cols), f32),
                   pltpu.VMEM((2 * NB, rows), f32),
                   pltpu.VMEM((2 * NB, cols), f32),
                   pltpu.VMEM((4, NB, LANES), f32)),
        in_specs=[pl.BlockSpec(memory_space=pl.ANY)],
        out_specs=(vmem, vmem, vmem, vmem),
        scratch_shapes=[
            pltpu.VMEM((rows, LANES), f32),
            pltpu.VMEM((NB, cols), f32),
            pltpu.VMEM((NB + 1, rs, LANES), f32),
            pltpu.VMEM((NB, cs, LANES), f32),
            pltpu.VMEM((NB, rs, LANES), f32),
            pltpu.VMEM((NB, rs, LANES), f32),
            pltpu.VMEM((NB, cs, LANES), f32),
            pltpu.VMEM((NB, cs, LANES), f32),
            pltpu.VMEM((rows, LANES), f32),
            pltpu.VMEM((cs, LANES), f32),
            pltpu.VMEM((rows, LANES), f32),
            pltpu.VMEM((NB, np_, 8 + cs, LANES), f32),
            pltpu.VMEM((NB, nq, 8 + rs, LANES), f32),
            pltpu.VMEM((rs, LANES), f32),
            dma((yc,)), dma, dma,
            dma((2, nq)), dma((2,)), dma((NB, np_)), dma((NB,)),
            dma((yc,)), dma((2, yc)), dma, dma((2,)),
        ],
        compiler_params=pltpu.CompilerParams(
            collective_id=0, has_side_effects=True, vmem_limit_bytes=20 * 1024 * 1024),
    )(matrix)


def pieces(x):
    hi = x.astype(jnp.bfloat16)
    rest = x - hi.astype(jnp.float32)
    mid = rest.astype(jnp.bfloat16)
    lo = (rest - mid.astype(jnp.float32)).astype(jnp.bfloat16)
    return hi, mid, lo


def update_kernel(a_ref, left_ref, right_ref, scal_ref, out_ref, coef_ref, left_p, right_p, slots, sems):
    me_p = lax.axis_index("prow")
    me_q = lax.axis_index("pcol")
    rows, cols = a_ref.shape
    depth, block = slots.shape[0], slots.shape[1]
    steps = rows // block
    dims = (((0,), (0,)), ((), ()))

    lh, lm, ll = pieces(left_ref[...])
    rh, rm, rl = pieces(right_ref[...])
    for k, (lp, rp) in enumerate(((lh, rh), (lh, rm), (lh, rl), (lm, rh), (lm, rm), (ll, rh))):
        left_p[2 * NB * k:2 * NB * (k + 1), :] = lp
        right_p[2 * NB * k:2 * NB * (k + 1), :] = rp
    lane = lax.broadcasted_iota(jnp.int32, (NB, LANES), 1)
    sub = lax.broadcasted_iota(jnp.int32, (NB, LANES), 0)
    for t in range(2):
        row = jnp.sum(jnp.where(lane == sub, scal_ref[2 + t], 0.0), axis=0, keepdims=True)
        coef_ref[t:t + 1, :] = row[:, 0:NB]

    def out_copy(step):
        slot = lax.rem(step, depth)
        part = pl.ds(pl.multiple_of(step * block, block), block)
        return pltpu.make_async_copy(slots.at[slot], out_ref.at[part, :], sems.at[slot])

    @pl.loop(0, steps)
    def _(step):
        slot = lax.rem(step, depth)
        part = pl.ds(pl.multiple_of(step * block, block), block)

        @pl.when(step >= depth)
        def _():
            out_copy(step - depth).wait()

        left = left_p[:, part]
        slots[slot] = a_ref[part, :] - lax.dot_general(
            left, right_p[...], dims, preferred_element_type=jnp.float32)
        k = left.shape[0]
        src = lax.broadcasted_iota(jnp.int32, (k, LANES), 0)
        lane = lax.broadcasted_iota(jnp.int32, (k, LANES), 1)
        pick = jnp.logical_and(
            lane < NB, (src == lane) | (src == lane + 6 * NB) | (src == lane + 10 * NB))
        vt = lax.dot_general(left, jnp.where(pick, 1.0, 0.0).astype(jnp.bfloat16), dims,
                             preferred_element_type=jnp.float32)
        stored = jnp.logical_and(me_q == 0, lax.broadcasted_iota(jnp.int32, (block, LANES), 1) < NB)
        slots[slot, :, 0:LANES] = jnp.where(stored, vt, slots[slot, :, 0:LANES])

        @pl.when(jnp.logical_and(me_p == 0, step == 0))
        def _():
            vt = slots[0, 0:NB, 0:LANES]
            slots[0, 0:NB, :] = right_ref[NB:, :]

            @pl.when(me_q == 0)
            def _():
                r = lax.broadcasted_iota(jnp.int32, (NB, LANES), 0)
                c = lax.broadcasted_iota(jnp.int32, (NB, LANES), 1)
                slots[0, 0:NB, 0:LANES] = jnp.where(
                    c < r, vt,
                    jnp.where(c == r, scal_ref[0], jnp.where(c == r + 1, scal_ref[1], right_ref[NB:, 0:LANES])))

        out_copy(step).start()

    @pl.loop(max(0, steps - depth), steps)
    def _(step):
        out_copy(step).wait()


def apply_panel(matrix, left, right, scal):
    rows, cols = matrix.shape
    block = min(rows, UPDATE_ROWS)
    depth = min(UPDATE_SLOTS, rows // block)
    vmem = pl.BlockSpec(memory_space=pltpu.VMEM)
    return pl.pallas_call(
        update_kernel,
        out_shape=(jax.ShapeDtypeStruct((rows, cols), jnp.float32),
                   jax.ShapeDtypeStruct((2, NB), jnp.float32)),
        in_specs=[vmem, vmem, vmem, vmem],
        out_specs=(pl.BlockSpec(memory_space=pl.ANY), vmem),
        scratch_shapes=[pltpu.VMEM((12 * NB, rows), jnp.bfloat16),
                        pltpu.VMEM((12 * NB, cols), jnp.bfloat16),
                        pltpu.VMEM((depth, block, cols), jnp.float32),
                        pltpu.SemaphoreType.DMA((depth,))],
        compiler_params=pltpu.CompilerParams(vmem_limit_bytes=20 * 1024 * 1024),
    )(matrix, left, right, scal)


def solution(mesh):
    np_, nq = mesh.shape["prow"], mesh.shape["pcol"]

    def per_device(matrix):
        return apply_panel(*reduce_panel(matrix, np_, nq))

    return jax.shard_map(
        per_device, mesh=mesh, in_specs=(P("prow", "pcol"),),
        out_specs=(P("prow", "pcol"), P()), check_vma=False)
```

```python
import functools

import jax
import jax.numpy as jnp
from jax import lax
from jax.experimental import pallas as pl
from jax.experimental.pallas import tpu as pltpu
from jax.sharding import PartitionSpec as P

NB = 8
EPS = 1e-06
LANES = 128
Y_PARTS = (1, 2, 2, 2, 1)
UPDATE_ROWS = 128
UPDATE_SLOTS = 6
BLOCKS = 4
MESH = pl.DeviceIdType.MESH


def householder(alpha, sumsq):
    beta = jnp.where(alpha >= 0.0, -1.0, 1.0) * jnp.sqrt(sumsq + EPS)
    return beta, (beta - alpha) / beta, alpha - beta


def lane_sum(x):
    return jnp.sum(x, axis=1, keepdims=True)


def total(x):
    return jnp.sum(lane_sum(x), axis=0, keepdims=True)


def y_chunks(cs):
    unit = cs // sum(Y_PARTS)
    sizes = [unit * part for part in Y_PARTS]
    return [(sum(sizes[:c]), n) for c, n in enumerate(sizes)]


def peers(me, n):
    if n & (n - 1):
        return [(d, lax.rem(me + d, n)) for d in range(1, n)]
    out = []
    for m in range(n - 1, 0, -1):
        other = me
        for b in range(n.bit_length() - 1):
            if m >> b & 1:
                other = other + (1 - 2 * lax.rem(me // (1 << b), 2)) * (1 << b)
        out.append((m, other))
    return out


def panel_kernel(np_, nq, a_hbm, a, left_o, right_o, scal_o,
                 strip, arows, colp, rowp, v_s, x_s, y_s, u_s, vb, ub, acc_s,
                 ybuf, xbuf, column_s,
                 a_sem, strip_sem, arow_sem, col_ssem, col_rsem, row_ssem, row_rsem,
                 y_ssem, y_rsem, x_ssem, x_rsem):
    me_p = lax.axis_index("prow")
    me_q = lax.axis_index("pcol")
    rows, cols = a.shape
    rs, cs = rows // LANES, cols // LANES
    ych = y_chunks(cs)
    groups = LANES // 8
    p_peers, q_peers = peers(me_p, np_), peers(me_q, nq)

    strip_cp = pltpu.make_async_copy(a_hbm.at[:, pl.ds(0, LANES)], strip, strip_sem)
    strip_cp.start()
    arow_cp = pltpu.make_async_copy(a_hbm.at[pl.ds(0, NB), :], arows, arow_sem)
    arow_cp.start()
    a_cps = []
    for c, (lo, n) in enumerate(ych):
        part = pl.ds(lo * LANES, n * LANES)
        a_cps.append(pltpu.make_async_copy(a_hbm.at[:, part], a.at[:, part], a_sem.at[c]))
    for cp in a_cps[:2]:
        cp.start()

    barrier = pltpu.get_barrier_semaphore()
    for d in range(1, np_):
        pl.semaphore_signal(barrier, inc=1, device_id={"prow": lax.rem(me_p + d, np_)}, device_id_type=MESH)
    for d in range(1, nq):
        pl.semaphore_signal(barrier, inc=1, device_id={"pcol": lax.rem(me_q + d, nq)}, device_id_type=MESH)
    pl.semaphore_wait(barrier, np_ + nq - 2)

    lane8 = lax.broadcasted_iota(jnp.int32, (8, LANES), 1)
    sub8 = lax.broadcasted_iota(jnp.int32, (8, LANES), 0)
    row_gl = (me_p * rows + lax.broadcasted_iota(jnp.int32, (rs, LANES), 0) * LANES
              + lax.broadcasted_iota(jnp.int32, (rs, LANES), 1))

    def col_gl(lo, n):
        return (me_q * cols + (lo + lax.broadcasted_iota(jnp.int32, (n, LANES), 0)) * LANES
                + lax.broadcasted_iota(jnp.int32, (n, LANES), 1))

    def col_copy(h, d):
        part = colp.at[pl.ds(0, 1)] if h == 0 else colp.at[pl.ds(1, NB)]
        return pltpu.make_async_remote_copy(
            src_ref=part, dst_ref=part, send_sem=col_ssem.at[h, d], recv_sem=col_rsem.at[h],
            device_id={"pcol": lax.rem(me_q + d, nq)}, device_id_type=MESH)

    def row_copy(i, d):
        return pltpu.make_async_remote_copy(
            src_ref=rowp.at[i], dst_ref=rowp.at[i], send_sem=row_ssem.at[i, d], recv_sem=row_rsem.at[i],
            device_id={"prow": lax.rem(me_p + d, np_)}, device_id_type=MESH)

    strip_cp.wait()

    @pl.when(me_q == 0)
    def _():
        @pl.loop(0, rs, unroll=min(8, rs))
        def _(s):
            t = strip[pl.ds(s * LANES, LANES), :].T
            for c in range(NB + 1):
                colp[c, pl.ds(s, 1), :] = t[c:c + 1, :]
        for h in range(2):
            for d in range(1, nq):
                col_copy(h, d).start()

    arow_cp.wait()

    @pl.when(me_p == 0)
    def _():
        for s in range(cs):
            blk = arows[:, s * LANES:(s + 1) * LANES]
            for i in range(NB):
                rowp[i, s:s + 1, :] = blk[i:i + 1, :]
        for i in range(2):
            for d in range(1, np_):
                row_copy(i, d).start()

    for cp in a_cps[2:]:
        cp.start()

    for ref in (v_s, x_s, y_s, u_s, left_o, right_o):
        ref[...] = jnp.zeros(ref.shape, jnp.float32)

    @pl.when(me_q != 0)
    def _():
        col_copy(0, 1).wait_recv()

    column_s[...] = colp[0]

    def y_part(c):
        lo, n = ych[c]
        return pl.ds(7, 1 + n) if c == 0 else pl.ds(8 + lo, n)

    def y_send(i, c):
        ref = ybuf.at[i, me_p, y_part(c), :]
        for m, peer in p_peers:
            pltpu.make_async_remote_copy(
                src_ref=ref, dst_ref=ref, send_sem=y_ssem.at[c], recv_sem=y_rsem.at[lax.rem(i, 2), c],
                device_id={"prow": peer}, device_id_type=MESH).start()

    def y_wait(i, c, sem):
        ref = ybuf.at[i, pl.ds(0, np_ - 1), y_part(c), :]
        pltpu.make_async_copy(ref, ref, sem).wait()

    def x_send(i):
        ref = xbuf.at[i, me_q, pl.ds(7, 1 + rs), :]
        for m, peer in q_peers:
            pltpu.make_async_remote_copy(
                src_ref=ref, dst_ref=ref, send_sem=x_ssem, recv_sem=x_rsem.at[lax.rem(i, 2)],
                device_id={"pcol": peer}, device_id_type=MESH).start()

    def x_wait(i, sem):
        ref = xbuf.at[i, pl.ds(0, nq - 1), pl.ds(7, 1 + rs), :]
        pltpu.make_async_copy(ref, ref, sem).wait()

    def scalar_row(first, second, vec, here, at):
        sums = [lane_sum(jnp.sum(ref[...] * vec[None], axis=1)) for ref in (first, second)]
        hit = jnp.logical_and(here, lane8 == at)
        sums += [lane_sum(jnp.where(hit, ref[:, 0, :], 0.0)) for ref in (first, second)]
        alpha = lane_sum(jnp.where(hit[0:1], vec[0:1], 0.0))
        sums.append(jnp.where(sub8[:, :1] == 0, alpha, total(vec * vec)))
        tile = jnp.zeros((8, LANES), jnp.float32)
        for k, one in enumerate(sums):
            tile = jnp.where(lane8 == sub8 + 8 * k, one, tile)
        return jnp.sum(tile, axis=0, keepdims=True)

    def unpack(buf, n):
        row = buf[0, 7:8, :]
        for p in range(1, n):
            row = row + buf[p, 7:8, :]
        row = jnp.broadcast_to(row, (8, LANES))
        return [jnp.broadcast_to(lane_sum(jnp.where(lane8 == sub8 + 8 * k, row, 0.0)), (8, LANES))
                for k in range(5)]

    def combine(coef_a, ref_a, coef_b, ref_b, lo, n):
        part = pl.ds(lo, n)
        acc = coef_a[0:1] * ref_a[0, part, :] + coef_b[0:1] * ref_b[0, part, :]
        for j in range(1, NB):
            acc = acc + (coef_a[j:j + 1] * ref_a[j, part, :] + coef_b[j:j + 1] * ref_b[j, part, :])
        return acc

    def spread(s):
        row = jnp.broadcast_to(column_s[s:s + 1, :], (8, LANES))
        return [jnp.broadcast_to(lane_sum(jnp.where(lane8 == sub8 + 8 * g, row, 0.0)), (8, LANES))
                for g in range(groups)]

    def y_finish(i, c, accs):
        lo, n = ych[c]
        for j in range(n):
            t = 8 + lo + j
            ybuf[i, me_p, t:t + 1, :] = jnp.sum(accs[j] + accs[n + j], axis=0, keepdims=True)
        y_send(i, c)

    def y_block(s, c, accs):
        lo, n = ych[c]
        accs = list(accs)
        for g in range(BLOCKS * groups):
            r = pl.ds(pl.multiple_of(s * (BLOCKS * LANES) + 8 * g, 8), 8)
            v = vb[r, :]
            for j in range(n):
                m = (g % 2) * n + j
                accs[m] = accs[m] + v * a[r, (lo + j) * LANES:(lo + j + 1) * LANES]
        return tuple(accs)

    def put(out, base, i, ref):
        for s in range(ref.shape[1]):
            part = slice(s * LANES, (s + 1) * LANES)
            row = jnp.broadcast_to(ref[i, s:s + 1, :], (NB, LANES))
            out[base:base + NB, part] = jnp.where(sub8 == i, row, out[base:base + NB, part])

    @pl.loop(0, NB)
    def _(i):
        masked = jnp.where(row_gl >= i, column_s[...], 0.0)
        unit_r = (row_gl == i).astype(jnp.float32)
        column_s[...] = masked

        @pl.when(i == 0)
        def _():
            a_cps[0].wait()

        ybuf[i, me_p, 7:8, :] = scalar_row(v_s, x_s, masked, me_p == 0, i)
        lo, n = ych[0]
        accs = [jnp.zeros((8, LANES), jnp.float32)] * (2 * n)
        for s in range(rs):
            for g, v in enumerate(spread(s)):
                r = pl.ds(s * LANES + 8 * g, 8)
                vb[r, :] = v
                for j in range(n):
                    m = (g % 2) * n + j
                    accs[m] = accs[m] + v * a[r, (lo + j) * LANES:(lo + j + 1) * LANES]
        for c in range(1, len(ych)):
            @pl.when(i == 0)
            def _(c=c):
                a_cps[c].wait()

            y_finish(i, c - 1, accs)
            zeros = (jnp.zeros((8, LANES), jnp.float32),) * (2 * ych[c][1])
            accs = lax.fori_loop(1, rs // BLOCKS, functools.partial(lambda s, t, c: y_block(s, c, t), c=c),
                                 y_block(0, c, zeros))
        y_finish(i, len(ych) - 1, accs)

        @pl.when(me_p != 0)
        def _():
            row_copy(i, 1).wait_recv()

        for c, (lo, n) in enumerate(ych):
            y_wait(i, c, y_rsem.at[lax.rem(i, 2), c])
            if c == 0:
                v_coef, x_coef, v_at, x_at, misc = unpack(ybuf.at[i], np_)
                beta, tau, denom = householder(misc[0:1], misc[1:2])
                inv = 1.0 / denom
                v_s[i] = (masked - beta * unit_r) * inv
                scal_o[0, pl.ds(i, 1), :] = beta
                scal_o[2, pl.ds(i, 1), :] = tau
            part, buf = pl.ds(lo, n), pl.ds(8 + lo, n)
            summed = ybuf[i, 0, buf, :]
            for p in range(1, np_):
                summed = summed + ybuf[i, p, buf, :]
            row_eff = rowp[i, part, :] - combine(v_at, y_s, x_at, u_s, lo, n)
            trans = (summed - combine(v_coef, y_s, x_coef, u_s, lo, n) - beta * row_eff) * inv
            mine = col_gl(lo, n) > i
            y_new = jnp.where(mine, tau * trans, 0.0)
            y_s[i, part, :] = y_new
            ub[part, :] = jnp.where(mine, row_eff - y_new, 0.0)
            us = [jnp.broadcast_to(ub[lo + j:lo + j + 1, :], (8, LANES)) for j in range(n)]

            def product(r, us=us, lo=lo, n=n):
                p = [us[k] * a[r, (lo + k) * LANES:(lo + k + 1) * LANES] for k in range(2)]
                for j in range(2, n):
                    p[j % 2] = p[j % 2] + us[j] * a[r, (lo + j) * LANES:(lo + j + 1) * LANES]
                return p[0] + p[1]

            if c < len(ych) - 1:
                @pl.loop(0, rs // BLOCKS)
                def _(s, c=c, product=product):
                    for g in range(BLOCKS * groups):
                        r = pl.ds(pl.multiple_of(s * (BLOCKS * LANES) + 8 * g, 8), 8)
                        acc_s[r, :] = product(r) if c == 0 else acc_s[r, :] + product(r)
            else:
                row_m = ub[...]
                xbuf[i, me_q, 7:8, :] = scalar_row(y_s, u_s, row_m, me_q == 0, i + 1)
                for s in range(rs):
                    tile = jnp.zeros((8, LANES), jnp.float32)
                    for g in range(groups):
                        r = pl.ds(s * LANES + 8 * g, 8)
                        tile = jnp.where(lane8 == sub8 + 8 * g, lane_sum(acc_s[r, :] + product(r)), tile)
                    xbuf[i, me_q, 8 + s:9 + s, :] = jnp.sum(tile, axis=0, keepdims=True)
                x_send(i)

        @pl.when(jnp.logical_and(me_p == 0, i < NB - 2))
        def _():
            for d in range(1, np_):
                row_copy(i + 2, d).start()

        @pl.when(jnp.logical_and(me_q != 0, i == 0))
        def _():
            col_copy(1, 1).wait_recv()

        for c in range(len(ych)):
            y_wait(i, c, y_ssem.at[c])
        put(left_o, 0, i, v_s)
        put(right_o, 0, i, y_s)

        @pl.when(i > 0)
        def _():
            put(left_o, NB, i - 1, x_s)
            put(right_o, NB, i - 1, u_s)

        unit_c = (col_gl(0, cs) == i + 1).astype(jnp.float32)
        x_wait(i, x_ssem)
        x_wait(i, x_rsem.at[lax.rem(i, 2)])
        y_coef, u_coef, y_at, u_at, misc2 = unpack(xbuf.at[i], nq)
        xsum = xbuf[i, 0, 8:8 + rs, :]
        for q in range(1, nq):
            xsum = xsum + xbuf[i, q, 8:8 + rs, :]
        beta2, tau2, denom2 = householder(misc2[0:1], misc2[1:2])
        col_next = colp[i + 1] - combine(y_at, v_s, u_at, x_s, 0, rs)
        inv2 = 1.0 / denom2
        prod = (xsum - combine(y_coef, v_s, u_coef, x_s, 0, rs) - beta2 * col_next) * inv2
        x_new = jnp.where(row_gl > i, tau2 * prod, 0.0)
        x_s[i] = x_new
        u_s[i] = (row_m - beta2 * unit_c) * inv2
        scal_o[1, pl.ds(i, 1), :] = beta2
        scal_o[3, pl.ds(i, 1), :] = tau2
        column_s[...] = col_next - x_new

    put(left_o, NB, NB - 1, x_s)
    put(right_o, NB, NB - 1, u_s)

    @pl.when(me_q == 0)
    def _():
        for h in range(2):
            for d in range(1, nq):
                col_copy(h, d).wait_send()

    @pl.when(me_p == 0)
    def _():
        @pl.loop(0, NB)
        def _(i):
            for d in range(1, np_):
                row_copy(i, d).wait_send()


def reduce_panel(matrix, np_, nq):
    rows, cols = matrix.shape
    rs, cs = rows // LANES, cols // LANES
    f32 = jnp.float32
    vmem = pl.BlockSpec(memory_space=pltpu.VMEM)
    dma = pltpu.SemaphoreType.DMA
    yc = len(Y_PARTS)
    return pl.pallas_call(
        functools.partial(panel_kernel, np_, nq),
        out_shape=(pltpu.VMEM((rows, cols), f32),
                   pltpu.VMEM((2 * NB, rows), f32),
                   pltpu.VMEM((2 * NB, cols), f32),
                   pltpu.VMEM((4, NB, LANES), f32)),
        in_specs=[pl.BlockSpec(memory_space=pl.ANY)],
        out_specs=(vmem, vmem, vmem, vmem),
        scratch_shapes=[
            pltpu.VMEM((rows, LANES), f32),
            pltpu.VMEM((NB, cols), f32),
            pltpu.VMEM((NB + 1, rs, LANES), f32),
            pltpu.VMEM((NB, cs, LANES), f32),
            pltpu.VMEM((NB, rs, LANES), f32),
            pltpu.VMEM((NB, rs, LANES), f32),
            pltpu.VMEM((NB, cs, LANES), f32),
            pltpu.VMEM((NB, cs, LANES), f32),
            pltpu.VMEM((rows, LANES), f32),
            pltpu.VMEM((cs, LANES), f32),
            pltpu.VMEM((rows, LANES), f32),
            pltpu.VMEM((NB, np_, 8 + cs, LANES), f32),
            pltpu.VMEM((NB, nq, 8 + rs, LANES), f32),
            pltpu.VMEM((rs, LANES), f32),
            dma((yc,)), dma, dma,
            dma((2, nq)), dma((2,)), dma((NB, np_)), dma((NB,)),
            dma((yc,)), dma((2, yc)), dma, dma((2,)),
        ],
        compiler_params=pltpu.CompilerParams(
            collective_id=0, has_side_effects=True, vmem_limit_bytes=20 * 1024 * 1024),
    )(matrix)


def pieces(x):
    hi = x.astype(jnp.bfloat16)
    rest = x - hi.astype(jnp.float32)
    mid = rest.astype(jnp.bfloat16)
    lo = (rest - mid.astype(jnp.float32)).astype(jnp.bfloat16)
    return hi, mid, lo


def update_kernel(a_ref, left_ref, right_ref, scal_ref, out_ref, coef_ref, left_p, right_p, slots, sems):
    me_p = lax.axis_index("prow")
    me_q = lax.axis_index("pcol")
    rows, cols = a_ref.shape
    depth, block = slots.shape[0], slots.shape[1]
    steps = rows // block
    dims = (((0,), (0,)), ((), ()))

    lh, lm, ll = pieces(left_ref[...])
    rh, rm, rl = pieces(right_ref[...])
    for k, (lp, rp) in enumerate(((lh, rh), (lh, rm), (lh, rl), (lm, rh), (lm, rm), (ll, rh))):
        left_p[2 * NB * k:2 * NB * (k + 1), :] = lp
        right_p[2 * NB * k:2 * NB * (k + 1), :] = rp
    lane = lax.broadcasted_iota(jnp.int32, (NB, LANES), 1)
    sub = lax.broadcasted_iota(jnp.int32, (NB, LANES), 0)
    for t in range(2):
        row = jnp.sum(jnp.where(lane == sub, scal_ref[2 + t], 0.0), axis=0, keepdims=True)
        coef_ref[t:t + 1, :] = row[:, 0:NB]

    def out_copy(step):
        slot = lax.rem(step, depth)
        part = pl.ds(pl.multiple_of(step * block, block), block)
        return pltpu.make_async_copy(slots.at[slot], out_ref.at[part, :], sems.at[slot])

    @pl.loop(0, steps)
    def _(step):
        slot = lax.rem(step, depth)
        part = pl.ds(pl.multiple_of(step * block, block), block)

        @pl.when(step >= depth)
        def _():
            out_copy(step - depth).wait()

        left = left_p[:, part]
        slots[slot] = a_ref[part, :] - lax.dot_general(
            left, right_p[...], dims, preferred_element_type=jnp.float32)
        k = left.shape[0]
        src = lax.broadcasted_iota(jnp.int32, (k, LANES), 0)
        lane = lax.broadcasted_iota(jnp.int32, (k, LANES), 1)
        pick = jnp.logical_and(
            lane < NB, (src == lane) | (src == lane + 6 * NB) | (src == lane + 10 * NB))
        vt = lax.dot_general(left, jnp.where(pick, 1.0, 0.0).astype(jnp.bfloat16), dims,
                             preferred_element_type=jnp.float32)
        stored = jnp.logical_and(me_q == 0, lax.broadcasted_iota(jnp.int32, (block, LANES), 1) < NB)
        slots[slot, :, 0:LANES] = jnp.where(stored, vt, slots[slot, :, 0:LANES])

        @pl.when(jnp.logical_and(me_p == 0, step == 0))
        def _():
            vt = slots[0, 0:NB, 0:LANES]
            slots[0, 0:NB, :] = right_ref[NB:, :]

            @pl.when(me_q == 0)
            def _():
                r = lax.broadcasted_iota(jnp.int32, (NB, LANES), 0)
                c = lax.broadcasted_iota(jnp.int32, (NB, LANES), 1)
                slots[0, 0:NB, 0:LANES] = jnp.where(
                    c < r, vt,
                    jnp.where(c == r, scal_ref[0], jnp.where(c == r + 1, scal_ref[1], right_ref[NB:, 0:LANES])))

        out_copy(step).start()

    @pl.loop(max(0, steps - depth), steps)
    def _(step):
        out_copy(step).wait()


def apply_panel(matrix, left, right, scal):
    rows, cols = matrix.shape
    block = min(rows, UPDATE_ROWS)
    depth = min(UPDATE_SLOTS, rows // block)
    vmem = pl.BlockSpec(memory_space=pltpu.VMEM)
    return pl.pallas_call(
        update_kernel,
        out_shape=(jax.ShapeDtypeStruct((rows, cols), jnp.float32),
                   jax.ShapeDtypeStruct((2, NB), jnp.float32)),
        in_specs=[vmem, vmem, vmem, vmem],
        out_specs=(pl.BlockSpec(memory_space=pl.ANY), vmem),
        scratch_shapes=[pltpu.VMEM((12 * NB, rows), jnp.bfloat16),
                        pltpu.VMEM((12 * NB, cols), jnp.bfloat16),
                        pltpu.VMEM((depth, block, cols), jnp.float32),
                        pltpu.SemaphoreType.DMA((depth,))],
        compiler_params=pltpu.CompilerParams(vmem_limit_bytes=20 * 1024 * 1024),
    )(matrix, left, right, scal)


def solution(mesh):
    np_, nq = mesh.shape["prow"], mesh.shape["pcol"]

    def per_device(matrix):
        return apply_panel(*reduce_panel(matrix, np_, nq))

    return jax.shard_map(
        per_device, mesh=mesh, in_specs=(P("prow", "pcol"),),
        out_specs=(P("prow", "pcol"), P()), check_vma=False)
```
